32 devices in a mesh: dp: 8 (over z, x), patch: 4 (over y, core).
Axes of the slice: x: 2, y: 2, z: 4, core: 2. Of those that a mesh axis runs over, the one named last changes fastest.
Arguments:
- token_ids: int32 [128], replicated, may hold values from 0 to 31999
- parents: int32 [128], replicated, may hold values from 0 to 3
- embedding: bfloat16 [32000, 1024], P('dp'), may hold values from -6 to 6
- self_gain: bfloat16 [1024], replicated, may hold values from 0.25 to 1.75
- query_weight: bfloat16 [1024, 1024], P(None, 'patch'), may hold values from -0.1875 to 0.1875
- key_weight: bfloat16 [1024, 1024], P(None, 'patch'), may hold values from -0.1875 to 0.1875
- value_weight: bfloat16 [1024, 1024], P(None, 'patch'), may hold values from -0.1875 to 0.1875
- output_weight: bfloat16 [1024, 1024], P('patch'), may hold values from -0.75 to 0.75
- past_keys: bfloat16 [128, 128, 1024], P('dp', None, 'patch'), may hold values from -200 to 200
- past_values: bfloat16 [128, 128, 1024], P('dp', None, 'patch'), may hold values from -6 to 6
- cross_gain: bfloat16 [1024], replicated, may hold values from 0.25 to 1.75
- cross_query: bfloat16 [1024, 1024], replicated, may hold values from -0.1875 to 0.1875
- cross_output: bfloat16 [1024, 1024], replicated, may hold values from -0.75 to 0.75
- image_keys: bfloat16 [8, 16, 256, 1024], P('dp', None, 'patch'), may hold values from -260 to 260
- image_values: bfloat16 [8, 16, 256, 1024], P('dp', None, 'patch'), may hold values from -6 to 6
Outputs:
- hidden: bfloat16 [128, 1024], P('dp')
- new_keys: bfloat16 [128, 1024], P('dp', 'patch')
- new_values: bfloat16 [128, 1024], P('dp', 'patch')
The draws below stay inside these ranges and needn't reach their ends.
Inputs may be any that keep to these rules, and one draw needn't show every extreme that they name: `parents`: a beam of the row's own image.
All inputs are finite; a program needn't handle non-finite values.
Results may differ from the reference program's by a relative error of at most 0.019.
The reference program's roundings to bfloat16 on the way count: a program that leaves them out, or rounds other values in their place, can miss the bound.
Values may be sent and summed in bfloat16 or wider, within the bound.
No kernel may reach another device: no remote copies, remote signals or barrier semaphores. Data moves between devices by JAX's collectives and lax.ppermute only.
A program may use at most 64 MiB of HBM per device.

```python
import math
import jax
import jax.numpy as jnp
import numpy as np
from jax import lax

D = 1024
HEADS = 16
PATCHES = 1024
VOCAB = 32000
BEAMS = 4
LEN = 128
IMG_DEV = 16
HD = 64
ROWS = 128
N_DP = 8


def loud_sample(key, array_shape, spread):
    key_base = jax.random.fold_in(key, 0)
    sample = spread * jnp.clip(jax.random.normal(key_base, array_shape, jnp.float32), -6.0, 6.0)
    return sample


def draw_past_keys(key, part):
    return loud_sample(jax.random.fold_in(key, 11), (ROWS, LEN, D), 1.5).astype(jnp.bfloat16)


def draw_image_keys(key, part):
    return loud_sample(jax.random.fold_in(key, 23), (N_DP, IMG_DEV, PATCHES // BEAMS, D), 2.0).astype(jnp.bfloat16)


def plant(values, own_key, low, top_value):
    dims = values.shape
    place = [jax.random.randint(jax.random.fold_in(own_key, axis), (), 0, dims[axis]) for axis in range(len(dims))]
    values = values.at[tuple(place)].set(low)
    longest = dims.index(max(dims))
    place[longest] = (place[longest] + 1) % dims[longest]
    return values.at[tuple(place)].set(top_value)


def steps_of(key, shape, cuts, smallest, high):
    loudness, own = 1.0, jax.random.fold_in(key, 6)
    for axis_at, parts in cuts:
        steps = jnp.exp(jax.random.uniform(jax.random.fold_in(own, axis_at), (parts,), jnp.float32, smallest / len(cuts), high / len(cuts)))
        loudness = loudness * jnp.repeat(steps, shape[axis_at] // parts).reshape([-1 if axis == axis_at else 1 for axis in range(len(shape))])
    return loudness


def rank_bounds(amount, lean):
    weights = [(1 << 20) // math.isqrt(standing ** lean) + 1 for standing in range(1, amount + 1)]
    width = 1 + sum(weights) // (1 << 30)
    return np.cumsum(np.array([max(1, weight // width) for weight in weights]))


def ranked_ids(key, dims, number_of, skew):
    table = rank_bounds(number_of, skew)
    lot = jax.random.randint(jax.random.fold_in(key, 1), dims, 0, int(table[number_of - 1]))
    standing = jnp.searchsorted(jnp.asarray(table, jnp.int32), lot, side="right")
    return jax.random.permutation(jax.random.fold_in(key, 2), number_of)[standing].astype(jnp.int32)


def centred(stream_key, shape, scale, limit, cuts=(), kind=jnp.bfloat16):
    values = scale * jax.random.normal(stream_key, shape, jnp.float32)
    if cuts:
        values = values * steps_of(stream_key, shape, cuts, -0.22, 0.18)
    return jnp.clip(values, -limit, limit).astype(kind)


def setup_inputs(seed: int = 0) -> dict:
    keys = jax.random.split(jax.random.key(seed), 16)
    token_ids = plant(ranked_ids(keys[0], (ROWS,), VOCAB, 2), jax.random.fold_in(keys[0], 3), 0, VOCAB - 1).astype(jnp.int32)
    parents = plant(jax.random.randint(keys[1], (ROWS,), 0, BEAMS), jax.random.fold_in(keys[1], 1), 0, BEAMS - 1).astype(jnp.int32)
    embedding = centred(keys[2], (VOCAB, D), 1.0, 6.0, ((0, 8),))
    self_gain = jnp.clip(1.0 + 0.15 * jax.random.normal(keys[3], (D,), jnp.float32), 0.25, 1.75).astype(jnp.bfloat16)
    query_weight = centred(keys[4], (D, D), D ** -0.5, 0.1875, ((1, 4),))
    key_weight = centred(keys[5], (D, D), D ** -0.5, 0.1875, ((1, 4),))
    value_weight = centred(keys[6], (D, D), D ** -0.5, 0.1875, ((1, 4),))
    output_weight = centred(keys[7], (D, D), HD ** -0.5, 0.75, ((0, 4),))
    past_keys = draw_past_keys(jax.random.fold_in(keys[15], 71), 0)
    past_values = centred(keys[9], (ROWS, LEN, D), 1.0, 6.0, ((0, 8), (2, 4)))
    cross_gain = jnp.clip(1.0 + 0.15 * jax.random.normal(keys[10], (D,), jnp.float32), 0.25, 1.75).astype(jnp.bfloat16)
    cross_query = centred(keys[11], (D, D), D ** -0.5, 0.1875)
    cross_output = centred(keys[12], (D, D), HD ** -0.5, 0.75)
    image_keys = draw_image_keys(jax.random.fold_in(keys[15], 71), 0)
    image_values = centred(keys[14], (N_DP, IMG_DEV, PATCHES // BEAMS, D), 1.0, 6.0, ((0, 8), (2, 4)))
    return {"token_ids": token_ids, "parents": parents, "embedding": embedding, "self_gain": self_gain, "query_weight": query_weight, "key_weight": key_weight, "value_weight": value_weight, "output_weight": output_weight, "past_keys": past_keys, "past_values": past_values, "cross_gain": cross_gain, "cross_query": cross_query, "cross_output": cross_output, "image_keys": image_keys, "image_values": image_values}


def normalize(inputs, gains):
    factor = lax.rsqrt(lax.optimization_barrier(jnp.mean(inputs * inputs, axis=-1, keepdims=True)) + 1e-06)
    return (inputs * factor * gains.astype(jnp.float32)).astype(jnp.bfloat16)

def soften(scores):
    maxima = lax.optimization_barrier(jnp.max(scores, axis=-1, keepdims=True))
    powers = jnp.exp(scores - maxima)
    totals = lax.optimization_barrier(jnp.sum(powers, axis=-1))
    rounded = lax.optimization_barrier(powers.astype(jnp.bfloat16)).astype(jnp.float32)
    return (rounded, totals)

def reference(token_ids, parents, embedding, self_gain, query_weight, key_weight, value_weight, output_weight, past_keys, past_values, cross_gain, cross_query, cross_output, image_keys, image_values):
    row_count = token_ids.shape[0]
    scaling = 1.0 / HD ** 0.5
    tokens = jnp.take(embedding, token_ids, axis=0).astype(jnp.float32)
    normed = normalize(tokens, self_gain)
    queries = jnp.dot(normed, query_weight, preferred_element_type=jnp.float32).astype(jnp.bfloat16)
    new_keys = jnp.dot(normed, key_weight, preferred_element_type=jnp.float32).astype(jnp.bfloat16)
    new_values = jnp.dot(normed, value_weight, preferred_element_type=jnp.float32).astype(jnp.bfloat16)
    row_index = jnp.arange(row_count, dtype=jnp.int32)
    stride = BEAMS * IMG_DEV
    source = row_index // stride * stride + parents.astype(jnp.int32) * IMG_DEV + row_index % IMG_DEV
    old_keys = jnp.take(past_keys, source, axis=0).astype(jnp.float32).reshape(row_count, LEN, HEADS, HD)
    old_values = jnp.take(past_values, source, axis=0).astype(jnp.float32).reshape(row_count, LEN, HEADS, HD)
    query_heads = queries.astype(jnp.float32).reshape(row_count, HEADS, HD)
    key_heads = new_keys.astype(jnp.float32).reshape(row_count, HEADS, HD)
    value_heads = new_values.astype(jnp.float32).reshape(row_count, HEADS, HD)
    scores = jnp.einsum('rhe,rlhe->rhl', query_heads, old_keys) * scaling
    own_score = lax.optimization_barrier(jnp.sum(query_heads * key_heads, axis=-1))[..., None] * scaling
    rounded, totals = soften(jnp.concatenate([scores, own_score], axis=-1))
    numerators = jnp.einsum('rhl,rlhe->rhe', rounded[..., :LEN], old_values) + rounded[..., LEN:] * value_heads
    self_context = (numerators / totals[..., None]).reshape(row_count, D).astype(jnp.bfloat16)
    middle = tokens + jnp.dot(self_context, output_weight, preferred_element_type=jnp.float32)
    probes = jnp.dot(normalize(middle, cross_gain), cross_query, preferred_element_type=jnp.float32).astype(jnp.bfloat16)
    groups = N_DP // BEAMS
    quarter = PATCHES // BEAMS
    probe_groups = probes.reshape(groups, BEAMS, IMG_DEV, HEADS, HD)
    key_groups = image_keys.reshape(groups, BEAMS, IMG_DEV, quarter, D)
    value_groups = image_values.reshape(groups, BEAMS, IMG_DEV, quarter, D)

    def one_group(pieces):
        probe_here, keys_here, values_here = pieces
        keys_here = jnp.transpose(keys_here.astype(jnp.float32), (1, 0, 2, 3)).reshape(IMG_DEV, PATCHES, HEADS, HD)
        values_here = jnp.transpose(values_here.astype(jnp.float32), (1, 0, 2, 3)).reshape(IMG_DEV, PATCHES, HEADS, HD)
        cross_scores = jnp.einsum('bihe,iphe->bihp', probe_here.astype(jnp.float32), keys_here) * scaling
        weights, sums = soften(cross_scores)
        summed = jnp.einsum('bihp,iphe->bihe', weights, values_here)
        return (summed / sums[..., None]).reshape(BEAMS * IMG_DEV, D).astype(jnp.bfloat16)
    cross_context = lax.map(one_group, (probe_groups, key_groups, value_groups)).reshape(row_count, D)
    hidden = (middle + jnp.dot(cross_context, cross_output, preferred_element_type=jnp.float32)).astype(jnp.bfloat16)
    return (hidden, new_keys, new_values)
```

```python
import functools
import math

import jax
import jax.numpy as jnp
from jax import lax
from jax.experimental import pallas as pl
from jax.experimental.pallas import tpu as pltpu
from jax.sharding import PartitionSpec as P

HEADS = 16
BEAMS = 4
SUB = 8
PAIR = SUB // BEAMS
LANES = 128
LOW = -1e30

f32 = jnp.float32
bf16 = jnp.bfloat16


def swap(value, axis, mask):
    pairs = [(source, source ^ mask) for source in range(lax.axis_size(axis))]
    return lax.ppermute(value, axis, pairs)


def params(mib):
    return pltpu.CompilerParams(vmem_limit_bytes=mib * 2**20)


def dot(a, b):
    return jnp.dot(a, b, preferred_element_type=f32)


def dot_nt(a, b):
    return lax.dot_general(a, b, (((1,), (1,)), ((), ())), preferred_element_type=f32)


def normalize(inputs, gains):
    factor = lax.rsqrt(jnp.mean(inputs * inputs, axis=-1, keepdims=True) + 1e-06)
    return (inputs * factor * gains.astype(f32)).astype(bf16)


def place():
    position = lax.axis_index("dp")
    return position // BEAMS, position % BEAMS, lax.axis_index("patch") % 2


def join_halves(own_ref, other_ref, core):
    own = own_ref[...].astype(f32)
    other = other_ref[...].astype(f32)
    return jnp.concatenate([jnp.where(core == 0, own, other), jnp.where(core == 0, other, own)], 0)


def gather_kernel(ids_ref, table_ref, *refs, groups, images, slab):
    outs, (blocks, sem) = refs[:-2], refs[-2:]
    group, _, core = place()
    first = lax.axis_index("dp") * slab
    here = images // 2
    rows = here * BEAMS
    width = blocks.shape[2]

    def local_id(k):
        slot, rest = k // rows, k % rows
        row = ((group ^ slot) * BEAMS + rest % BEAMS) * images + core * here + rest // BEAMS
        return ids_ref[row] - first

    def start(k, carry):
        held = jnp.clip(local_id(k), 0, slab - 1)
        pltpu.make_async_copy(table_ref.at[held // SUB], blocks.at[k], sem).start()
        return carry

    lax.fori_loop(0, groups * rows, start, 0, unroll=SUB)
    pltpu.make_async_copy(blocks, blocks, sem).wait()
    sub = lax.broadcasted_iota(jnp.int32, (SUB, width), 0)
    for slot in range(groups):
        for base in range(0, rows, 2 * SUB):
            tiles = []
            for tile in (base, base + SUB):
                packed = jnp.zeros((SUB, width), f32)
                for k in range(SUB):
                    at = slot * rows + tile + k
                    local = local_id(at)
                    mine = jnp.logical_and(local >= 0, local < slab)
                    place_in = jnp.clip(local, 0, slab - 1) % SUB
                    turned = pltpu.roll(blocks[at].astype(f32), (k + SUB - place_in) % SUB, 0)
                    packed = jnp.where(jnp.logical_and(sub == k, mine), turned, packed)
                tiles.append(packed)
            outs[slot][base : base + 2 * SUB, :] = jnp.concatenate(tiles, 0).astype(bf16)


def spread(rows8, heads, head_size):
    owner = lax.broadcasted_iota(jnp.int32, rows8.shape, 1) // head_size
    return jnp.concatenate([jnp.where(owner == h, rows8, 0.0) for h in range(heads)], 0)


def fold(wide, heads, head_size):
    owner = lax.broadcasted_iota(jnp.int32, (SUB, wide.shape[1]), 1) // head_size
    folded = wide[:SUB]
    for h in range(1, heads):
        folded = jnp.where(owner == h, wide[h * SUB : (h + 1) * SUB], folded)
    return folded


def same_image(shape, length):
    row = lax.broadcasted_iota(jnp.int32, shape, 0) % SUB // BEAMS
    return row == lax.broadcasted_iota(jnp.int32, shape, 1) // length


def self_kernel(parents_ref, own_ref, other_ref, gain_ref, wq_ref, wk_ref, wv_ref, pk_ref, pv_ref,
                context_ref, key_ref, value_ref, key_scr, value_scr, *, head_size):
    group, beam, core = place()
    images, length, width = pk_ref.shape
    heads = width // head_size
    scaling = 1.0 / math.sqrt(head_size)
    normed = normalize(join_halves(own_ref, other_ref, core), gain_ref[...])
    queries = dot(normed, wq_ref[...]).astype(bf16).astype(f32)
    keys = dot(normed, wk_ref[...]).astype(bf16).astype(f32)
    values = dot(normed, wv_ref[...]).astype(bf16).astype(f32)
    for first in range(0, width, LANES):
        key_scr[first // LANES] = keys[:, first : first + LANES]
        value_scr[first // LANES] = values[:, first : first + LANES]
    for first in range(0, width, LANES):
        mine = pl.ds(beam, images, stride=BEAMS)
        key_ref[:, first : first + LANES] = key_scr[first // LANES, mine, :].astype(bf16)
        value_ref[:, first : first + LANES] = value_scr[first // LANES, mine, :].astype(bf16)
    sub = lax.broadcasted_iota(jnp.int32, (SUB, width), 0)
    pairs = images // PAIR
    seen = same_image((heads * SUB, PAIR * length), length)
    scores, owns = [], []
    for j in range(pairs):
        q = spread(queries[j * SUB : (j + 1) * SUB], heads, head_size)
        k = jnp.concatenate([keys[j * SUB : (j + 1) * SUB]] * heads, 0)
        past = pk_ref[j * PAIR : (j + 1) * PAIR].reshape(PAIR * length, width)
        scores.append(dot_nt(q.astype(bf16), past))
        owns.append(jnp.sum(q * k, axis=-1, keepdims=True) * scaling)
    weights, own_weights, totals = [], [], []
    for j in range(pairs):
        s = jnp.where(seen, scores[j] * scaling, LOW)
        peak = jnp.maximum(jnp.max(s, axis=-1, keepdims=True), owns[j])
        power = jnp.exp(s - peak)
        own_power = jnp.exp(owns[j] - peak)
        totals.append(jnp.sum(power, axis=-1, keepdims=True) + own_power)
        weights.append(power.astype(bf16))
        own_weights.append(own_power.astype(bf16).astype(f32))
    done = []
    for j in range(pairs):
        past = pv_ref[j * PAIR : (j + 1) * PAIR].reshape(PAIR * length, width)
        v = jnp.concatenate([values[j * SUB : (j + 1) * SUB]] * heads, 0)
        summed = (dot(weights[j], past) + own_weights[j] * v) / totals[j]
        folded = fold(summed, heads, head_size)
        lives = jnp.zeros((SUB, width), jnp.int32)
        for k in range(SUB):
            row = (group * BEAMS + k % BEAMS) * images + j * PAIR + k // BEAMS
            lives = jnp.where(sub == k, (parents_ref[row] == beam).astype(jnp.int32), lives)
        done.append(jnp.where(lives > 0, folded, 0.0))
    context_ref[...] = jnp.concatenate(done, 0).astype(bf16)


def cross_kernel(*refs, pieces, head_size):
    contexts = refs[:pieces]
    outputs = refs[pieces : 2 * pieces]
    own_ref, other_ref, gain_ref, query_ref, ik_ref, iv_ref = refs[2 * pieces : 2 * pieces + 6]
    middle_ref, *messages = refs[2 * pieces + 6 : 2 * pieces + 7 + BEAMS]
    mid_scr, sum_scr, s_scr, p_scr = refs[2 * pieces + 7 + BEAMS :]
    _, beam, core = place()
    _, images, length, width = ik_ref.shape
    scaling = 1.0 / math.sqrt(head_size)
    middle = join_halves(own_ref, other_ref, core)
    for piece in range(pieces):
        middle = middle + dot(contexts[piece][...], outputs[piece][...])
    mine = pl.ds(beam, images, stride=BEAMS)
    for first in range(0, width, LANES):
        mid_scr[first // LANES] = middle[:, first : first + LANES]
    for first in range(0, width, LANES):
        middle_ref[:, first : first + LANES] = mid_scr[first // LANES, mine, :]
    probes = dot(normalize(middle, gain_ref[...]), query_ref[...]).astype(bf16).astype(f32)
    pairs = images // PAIR
    block = min(width, 2 * LANES)
    heads = block // head_size
    blocks = width // block
    rows = heads * SUB
    for j in range(pairs):
        for n in range(blocks):
            at = slice(n * block, (n + 1) * block)
            q = spread(probes[j * SUB : (j + 1) * SUB, at], heads, head_size).astype(bf16)
            past = ik_ref[0, j * PAIR : (j + 1) * PAIR, :, at].reshape(PAIR * length, block)
            s_scr[(j * blocks + n) * rows : (j * blocks + n + 1) * rows, :] = dot_nt(q, past)
    seen = same_image((rows, PAIR * length), length)
    lane = lax.broadcasted_iota(jnp.int32, (SUB, LANES), 1)
    for j in range(pairs):
        stats = jnp.zeros((SUB, LANES), f32)
        for n in range(blocks):
            at = slice((j * blocks + n) * rows, (j * blocks + n + 1) * rows)
            s = jnp.where(seen, s_scr[at, :] * scaling, LOW)
            peak = jnp.max(s, axis=-1, keepdims=True)
            power = jnp.exp(s - peak)
            total = jnp.sum(power, axis=-1, keepdims=True)
            p_scr[at, :] = power.astype(bf16)
            for h in range(heads):
                head = n * heads + h
                stats = jnp.where(lane == head, peak[h * SUB : (h + 1) * SUB], stats)
                stats = jnp.where(lane == HEADS + head, total[h * SUB : (h + 1) * SUB], stats)
        sum_scr[width // LANES, j * SUB : (j + 1) * SUB, :] = stats
    for j in range(pairs):
        for n in range(blocks):
            at = slice((j * blocks + n) * rows, (j * blocks + n + 1) * rows)
            past = iv_ref[0, j * PAIR : (j + 1) * PAIR, :, n * block : (n + 1) * block]
            summed = fold(dot(p_scr[at, :], past.reshape(PAIR * length, block)), heads, head_size)
            for part in range(block // LANES):
                sum_scr[n * (block // LANES) + part, j * SUB : (j + 1) * SUB, :] = summed[
                    :, part * LANES : (part + 1) * LANES
                ]
    for k in range(BEAMS):
        theirs = pl.ds(beam ^ k, images, stride=BEAMS)
        for part in range(width // LANES + 1):
            messages[k][:, part * LANES : (part + 1) * LANES] = sum_scr[part, theirs, :]


def merge(parts, head_size):
    width = parts[0].shape[1] - LANES
    lane = lax.broadcasted_iota(jnp.int32, (1, LANES), 1)
    stats = [part[:, width:] for part in parts]
    peak = functools.reduce(jnp.maximum, stats)
    row = lax.broadcasted_iota(jnp.int32, (LANES, width), 0)
    owner = lax.broadcasted_iota(jnp.int32, (LANES, width), 1) // head_size
    widen = (row == owner).astype(f32)
    total = 0.0
    sums = 0.0
    for part, stat in zip(parts, stats):
        scale = jnp.where(lane < HEADS, jnp.exp(stat - peak), 0.0)
        total = total + pltpu.roll(stat, LANES - HEADS, 1) * scale
        sums = sums + part[:, :width] * jnp.dot(scale, widen, precision=lax.Precision.HIGHEST)
    return sums, peak, total, lane, widen


def merge_kernel(*refs, head_size):
    parts, out_ref = [ref[...] for ref in refs[:-1]], refs[-1]
    sums, peak, total, lane, _ = merge(parts, head_size)
    width = sums.shape[1]
    out_ref[:, :width] = sums
    out_ref[:, width:] = jnp.where(lane < HEADS, peak, pltpu.roll(total, HEADS, 1))


def final_kernel(*refs, head_size):
    parts = [ref[...] for ref in refs[:-3]]
    middle_ref, weight_ref, out_ref = refs[-3:]
    sums, _, total, lane, widen = merge(parts, head_size)
    total = jnp.where(lane < HEADS, total, 1.0)
    wide = jnp.dot(total, widen, precision=lax.Precision.HIGHEST)
    context = (sums / wide).astype(bf16)
    out_ref[...] = (middle_ref[...] + dot(context, weight_ref[...])).astype(bf16)


def shards(
    token_ids,
    parents,
    embedding,
    self_gain,
    query_weight,
    key_weight,
    value_weight,
    output_weight,
    past_keys,
    past_values,
    cross_gain,
    cross_query,
    cross_output,
    image_keys,
    image_values,
):
    images, length, width_here = past_keys.shape
    slab, width = embedding.shape
    head_size = width // HEADS
    groups = lax.axis_size("dp") // BEAMS
    patches = lax.axis_size("patch")
    group_rows = BEAMS * images
    half = group_rows // 2
    smem = pl.BlockSpec(memory_space=pltpu.SMEM)
    vmem = pl.BlockSpec(memory_space=pltpu.VMEM)

    outputs = [output_weight]
    mask = 1
    while mask < patches:
        outputs = outputs + [swap(piece, "patch", mask) for piece in outputs]
        mask *= 2

    slots = pl.pallas_call(
        functools.partial(gather_kernel, groups=groups, images=images, slab=slab),
        out_shape=[jax.ShapeDtypeStruct((half, width), bf16)] * groups,
        in_specs=[smem, pl.BlockSpec(memory_space=pl.ANY)],
        out_specs=[vmem] * groups,
        scratch_shapes=[
            pltpu.VMEM((groups * half, SUB, width), bf16),
            pltpu.SemaphoreType.DMA,
        ],
        compiler_params=params(16),
        name="gather",
    )(token_ids, embedding.reshape(slab // SUB, SUB, width))
    while len(slots) > 1:
        keep = len(slots) // 2
        slots = [a + swap(b, "dp", keep * BEAMS) for a, b in zip(slots[:keep], slots[keep:])]
    own = slots[0]
    own = own + swap(own, "dp", 1) + swap(own, "dp", 2) + swap(own, "dp", 3)
    other = swap(own, "patch", 1)

    context, new_key, new_value = pl.pallas_call(
        functools.partial(self_kernel, head_size=head_size),
        out_shape=[
            jax.ShapeDtypeStruct((group_rows, width_here), bf16),
            jax.ShapeDtypeStruct((images, width_here), bf16),
            jax.ShapeDtypeStruct((images, width_here), bf16),
        ],
        in_specs=[smem] + [vmem] * 8,
        out_specs=[vmem] * 3,
        scratch_shapes=[pltpu.VMEM((width_here // LANES, group_rows, LANES), f32)] * 2,
        compiler_params=params(16),
        name="self_attention",
    )(parents, own, other, self_gain.reshape(1, width), query_weight, key_weight, value_weight,
      past_keys, past_values)
    context = context + swap(context, "dp", 1) + swap(context, "dp", 2) + swap(context, "dp", 3)
    contexts = [context] + [swap(context, "patch", k) for k in range(1, patches)]

    patch_count = image_keys.shape[2]
    score_rows = images // PAIR * HEADS * SUB
    middle, *messages = pl.pallas_call(
        functools.partial(cross_kernel, pieces=patches, head_size=head_size),
        out_shape=[jax.ShapeDtypeStruct((images, width), f32)]
        + [jax.ShapeDtypeStruct((images, width + LANES), f32)] * BEAMS,
        in_specs=[vmem] * (2 * patches + 6),
        out_specs=[vmem] * (1 + BEAMS),
        scratch_shapes=[
            pltpu.VMEM((width // LANES, group_rows, LANES), f32),
            pltpu.VMEM((width // LANES + 1, group_rows, LANES), f32),
            pltpu.VMEM((score_rows, PAIR * patch_count), f32),
            pltpu.VMEM((score_rows, PAIR * patch_count), bf16),
        ],
        compiler_params=params(24),
        name="cross_attention",
    )(*contexts, *outputs, own, other, cross_gain.reshape(1, width), cross_query, image_keys,
      image_values)
    parts = [messages[0]] + [swap(messages[k], "dp", k) for k in range(1, BEAMS)]
    part = pl.pallas_call(
        functools.partial(merge_kernel, head_size=head_size),
        out_shape=jax.ShapeDtypeStruct((images, width + LANES), f32),
        in_specs=[vmem] * BEAMS,
        out_specs=vmem,
        compiler_params=params(8),
        name="merge",
    )(*parts)
    parts = [part] + [swap(part, "patch", k) for k in range(1, patches)]
    hidden = pl.pallas_call(
        functools.partial(final_kernel, head_size=head_size),
        out_shape=jax.ShapeDtypeStruct((images, width), bf16),
        in_specs=[vmem] * (patches + 2),
        out_specs=vmem,
        compiler_params=params(8),
        name="final",
    )(*parts, middle, cross_output)
    return (hidden, new_key, new_value)


def solution(mesh):
    in_specs = (
        P(),
        P(),
        P("dp", None),
        P(),
        P(None, "patch"),
        P(None, "patch"),
        P(None, "patch"),
        P("patch", None),
        P("dp", None, "patch"),
        P("dp", None, "patch"),
        P(),
        P(),
        P(),
        P("dp", None, "patch", None),
        P("dp", None, "patch", None),
    )
    out_specs = (P("dp", None), P("dp", "patch"), P("dp", "patch"))
    return jax.shard_map(shards, mesh=mesh, in_specs=in_specs, out_specs=out_specs, check_vma=False)
```

```python
import functools
import math

import jax
import jax.numpy as jnp
from jax import lax
from jax.experimental import pallas as pl
from jax.experimental.pallas import tpu as pltpu
from jax.sharding import PartitionSpec as P


HEADS = 16
BEAMS = 4
SUB = 8
PAIR = SUB // BEAMS
LANES = 128
LOW = -1e30

f32 = jnp.float32
bf16 = jnp.bfloat16


def swap(value, axis, mask):
    pairs = [(source, source ^ mask) for source in range(lax.axis_size(axis))]
    return lax.ppermute(value, axis, pairs)


def params(mib):
    return pltpu.CompilerParams(vmem_limit_bytes=mib * 2**20)


def dot(a, b):
    return jnp.dot(a, b, preferred_element_type=f32)


def dot_nt(a, b):
    return lax.dot_general(a, b, (((1,), (1,)), ((), ())), preferred_element_type=f32)


def normalize(inputs, gains):
    factor = lax.rsqrt(jnp.mean(inputs * inputs, axis=-1, keepdims=True) + 1e-06)
    return (inputs * factor * gains.astype(f32)).astype(bf16)


def place():
    position = lax.axis_index("dp")
    return position // BEAMS, position % BEAMS, lax.axis_index("patch") % 2


def join_halves(own_ref, other_ref, core):
    own = own_ref[...].astype(f32)
    other = other_ref[...].astype(f32)
    return jnp.concatenate([jnp.where(core == 0, own, other), jnp.where(core == 0, other, own)], 0)


def gather_kernel(ids_ref, table_ref, *refs, slots, images, slab):
    outs, (ids_smem, blocks, ids_sem, sem) = refs[:-4], refs[-4:]
    pltpu.make_async_copy(ids_ref, ids_smem, ids_sem).start()
    group, _, core = place()
    first = lax.axis_index("dp") * slab
    here = images // 2
    rows = here * BEAMS
    width = blocks.shape[2]
    locals_, mine = [], []
    pltpu.make_async_copy(ids_ref, ids_smem, ids_sem).wait()
    for slot in slots:
        base = (group ^ slot) * (BEAMS * images) + core * here
        for k in range(rows):
            local = ids_smem[base + (k % BEAMS) * images + k // BEAMS] - first
            held = jnp.clip(local, 0, slab - 1)
            source = table_ref.at[lax.shift_right_logical(held, int(math.log2(SUB)))]
            pltpu.make_async_copy(source, blocks.at[len(mine)], sem).start()
            locals_.append(held & (SUB - 1))
            mine.append(local == held)
    pltpu.make_async_copy(blocks, blocks, sem).wait()
    sub = lax.broadcasted_iota(jnp.int32, (SUB, width), 0)
    for out, begin in zip(outs, range(0, len(mine), rows)):
        for base in range(0, rows, 2 * SUB):
            tiles = []
            for tile in (base, base + SUB):
                packed = jnp.zeros((SUB, width), f32)
                for k in range(SUB):
                    at = begin + tile + k
                    turned = pltpu.roll(blocks[at].astype(f32), (k + SUB - locals_[at]) & (SUB - 1), 0)
                    packed = jnp.where(jnp.logical_and(sub == k, mine[at]), turned, packed)
                tiles.append(packed)
            out[base : base + 2 * SUB, :] = jnp.concatenate(tiles, 0).astype(bf16)


def spread(rows8, heads, head_size):
    owner = lax.broadcasted_iota(jnp.int32, rows8.shape, 1) // head_size
    return jnp.concatenate([jnp.where(owner == h, rows8, 0.0) for h in range(heads)], 0)


def fold(wide, heads, head_size):
    owner = lax.broadcasted_iota(jnp.int32, (SUB, wide.shape[1]), 1) // head_size
    folded = wide[:SUB]
    for h in range(1, heads):
        folded = jnp.where(owner == h, wide[h * SUB : (h + 1) * SUB], folded)
    return folded


def same_image(shape, length):
    row = lax.broadcasted_iota(jnp.int32, shape, 0) % SUB // BEAMS
    return row == lax.broadcasted_iota(jnp.int32, shape, 1) // length


def self_kernel(parents_ref, own_ref, other_ref, gain_ref, wq_ref, wk_ref, wv_ref, pk_ref, pv_ref,
                context_ref, key_ref, value_ref, key_scr, value_scr, *, head_size):
    group, beam, core = place()
    images, length, width = pk_ref.shape
    heads = width // head_size
    scaling = 1.0 / math.sqrt(head_size)
    normed = normalize(join_halves(own_ref, other_ref, core), gain_ref[...])
    queries = dot(normed, wq_ref[...]).astype(bf16).astype(f32)
    keys = dot(normed, wk_ref[...]).astype(bf16).astype(f32)
    values = dot(normed, wv_ref[...]).astype(bf16).astype(f32)
    for first in range(0, width, LANES):
        key_scr[first // LANES] = keys[:, first : first + LANES]
        value_scr[first // LANES] = values[:, first : first + LANES]
    for first in range(0, width, LANES):
        mine = pl.ds(beam, images, stride=BEAMS)
        key_ref[:, first : first + LANES] = key_scr[first // LANES, mine, :].astype(bf16)
        value_ref[:, first : first + LANES] = value_scr[first // LANES, mine, :].astype(bf16)
    sub = lax.broadcasted_iota(jnp.int32, (SUB, width), 0)
    pairs = images // PAIR
    seen = same_image((heads * SUB, PAIR * length), length)
    scores, owns = [], []
    for j in range(pairs):
        q = spread(queries[j * SUB : (j + 1) * SUB], heads, head_size)
        k = jnp.concatenate([keys[j * SUB : (j + 1) * SUB]] * heads, 0)
        past = pk_ref[j * PAIR : (j + 1) * PAIR].reshape(PAIR * length, width)
        scores.append(dot_nt(q.astype(bf16), past))
        owns.append(jnp.sum(q * k, axis=-1, keepdims=True) * scaling)
    weights, own_weights, totals = [], [], []
    for j in range(pairs):
        s = jnp.where(seen, scores[j] * scaling, LOW)
        peak = jnp.maximum(jnp.max(s, axis=-1, keepdims=True), owns[j])
        power = jnp.exp(s - peak)
        own_power = jnp.exp(owns[j] - peak)
        totals.append(jnp.sum(power, axis=-1, keepdims=True) + own_power)
        weights.append(power.astype(bf16))
        own_weights.append(own_power.astype(bf16).astype(f32))
    done = []
    for j in range(pairs):
        past = pv_ref[j * PAIR : (j + 1) * PAIR].reshape(PAIR * length, width)
        v = jnp.concatenate([values[j * SUB : (j + 1) * SUB]] * heads, 0)
        summed = (dot(weights[j], past) + own_weights[j] * v) / totals[j]
        folded = fold(summed, heads, head_size)
        lives = jnp.zeros((SUB, width), jnp.int32)
        for k in range(SUB):
            row = (group * BEAMS + k % BEAMS) * images + j * PAIR + k // BEAMS
            lives = jnp.where(sub == k, (parents_ref[row] == beam).astype(jnp.int32), lives)
        done.append(jnp.where(lives > 0, folded, 0.0))
    context_ref[...] = jnp.concatenate(done, 0).astype(bf16)


def cross_kernel(*refs, pieces, head_size):
    contexts = refs[:pieces]
    outputs = refs[pieces : 2 * pieces]
    own_ref, other_ref, gain_ref, query_ref, ik_ref, iv_ref = refs[2 * pieces : 2 * pieces + 6]
    middle_ref, *messages = refs[2 * pieces + 6 : 2 * pieces + 7 + BEAMS]
    mid_scr, sum_scr, s_scr, p_scr = refs[2 * pieces + 7 + BEAMS :]
    _, beam, core = place()
    _, images, length, width = ik_ref.shape
    scaling = 1.0 / math.sqrt(head_size)
    middle = join_halves(own_ref, other_ref, core)
    for piece in range(pieces):
        middle = middle + dot(contexts[piece][...], outputs[piece][...])
    mine = pl.ds(beam, images, stride=BEAMS)
    for first in range(0, width, LANES):
        mid_scr[first // LANES] = middle[:, first : first + LANES]
    for first in range(0, width, LANES):
        middle_ref[:, first : first + LANES] = mid_scr[first // LANES, mine, :]
    probes = dot(normalize(middle, gain_ref[...]), query_ref[...]).astype(bf16).astype(f32)
    pairs = images // PAIR
    block = min(width, 2 * LANES)
    heads = block // head_size
    blocks = width // block
    rows = heads * SUB
    for j in range(pairs):
        for n in range(blocks):
            at = slice(n * block, (n + 1) * block)
            q = spread(probes[j * SUB : (j + 1) * SUB, at], heads, head_size).astype(bf16)
            past = ik_ref[0, j * PAIR : (j + 1) * PAIR, :, at].reshape(PAIR * length, block)
            s_scr[(j * blocks + n) * rows : (j * blocks + n + 1) * rows, :] = dot_nt(q, past)
    seen = same_image((rows, PAIR * length), length)
    lane = lax.broadcasted_iota(jnp.int32, (SUB, LANES), 1)
    for j in range(pairs):
        stats = jnp.zeros((SUB, LANES), f32)
        for n in range(blocks):
            at = slice((j * blocks + n) * rows, (j * blocks + n + 1) * rows)
            s = jnp.where(seen, s_scr[at, :] * scaling, LOW)
            peak = jnp.max(s, axis=-1, keepdims=True)
            power = jnp.exp(s - peak)
            total = jnp.sum(power, axis=-1, keepdims=True)
            p_scr[at, :] = power.astype(bf16)
            for h in range(heads):
                head = n * heads + h
                stats = jnp.where(lane == head, peak[h * SUB : (h + 1) * SUB], stats)
                stats = jnp.where(lane == HEADS + head, total[h * SUB : (h + 1) * SUB], stats)
        sum_scr[width // LANES, j * SUB : (j + 1) * SUB, :] = stats
    for j in range(pairs):
        for n in range(blocks):
            at = slice((j * blocks + n) * rows, (j * blocks + n + 1) * rows)
            past = iv_ref[0, j * PAIR : (j + 1) * PAIR, :, n * block : (n + 1) * block]
            summed = fold(dot(p_scr[at, :], past.reshape(PAIR * length, block)), heads, head_size)
            for part in range(block // LANES):
                sum_scr[n * (block // LANES) + part, j * SUB : (j + 1) * SUB, :] = summed[
                    :, part * LANES : (part + 1) * LANES
                ]
    for k in range(BEAMS):
        theirs = pl.ds(beam ^ k, images, stride=BEAMS)
        for part in range(width // LANES):
            messages[k][:, part * LANES : (part + 1) * LANES] = sum_scr[part, theirs, :].astype(bf16)
        messages[k][:, width:] = pack(sum_scr[width // LANES, theirs, :])


def split(value, terms):
    out = []
    for _ in range(terms):
        out.append(value.astype(bf16))
        value = value - out[-1].astype(f32)
    return out


def pack(stats):
    lane = lax.broadcasted_iota(jnp.int32, stats.shape, 1)
    packed = jnp.zeros(stats.shape, f32)
    for at, term in enumerate(split(stats, 3)):
        term = term.astype(f32)
        tall = pltpu.roll(term, 2 * at * HEADS, 1) if at else term
        inside = jnp.logical_and(lane >= 2 * at * HEADS, lane < 2 * (at + 1) * HEADS)
        packed = jnp.where(inside, tall, packed)
    return packed.astype(bf16)


def merge(parts, head_size, last):
    rows = parts[0].shape[0]
    width = parts[0].shape[1] - LANES
    lane = lax.broadcasted_iota(jnp.int32, (rows, LANES), 1)
    peaks, totals = [], []
    for part in parts:
        stat = part[:, width:].astype(f32)
        stat = stat + pltpu.roll(stat, LANES - 2 * HEADS, 1) + pltpu.roll(stat, LANES - 4 * HEADS, 1)
        peaks.append(stat)
        totals.append(pltpu.roll(stat, LANES - HEADS, 1))
    peak = functools.reduce(jnp.maximum, peaks)
    scales = [jnp.where(lane < HEADS, jnp.exp(p - peak), 0.0) for p in peaks]
    total = sum(scale * t for scale, t in zip(scales, totals))
    if last:
        total = jnp.where(lane < HEADS, total, 1.0)
        scales = [scale / total for scale in scales]
    row = lax.broadcasted_iota(jnp.int32, (LANES, width), 0)
    owner = lax.broadcasted_iota(jnp.int32, (LANES, width), 1) // head_size
    widen = (row == owner).astype(bf16)
    high, low = split(jnp.concatenate(scales, 0), 2)
    wide = dot(jnp.concatenate([high, low], 0), widen)
    many = len(parts) * rows
    wide = wide[:many] + wide[many:]
    sums = 0.0
    for k, part in enumerate(parts):
        sums = sums + part[:, :width].astype(f32) * wide[k * rows : (k + 1) * rows]
    stats = jnp.where(lane < HEADS, peak, pltpu.roll(total, HEADS, 1))
    return sums, jnp.where(lane < 2 * HEADS, stats, 0.0)


def merge_kernel(*refs, head_size):
    parts, out_ref = [ref[...] for ref in refs[:-1]], refs[-1]
    sums, stats = merge(parts, head_size, False)
    width = sums.shape[1]
    out_ref[:, :width] = sums.astype(bf16)
    out_ref[:, width:] = pack(stats)


def final_kernel(*refs, head_size):
    parts = [ref[...] for ref in refs[:-3]]
    middle_ref, weight_ref, out_ref = refs[-3:]
    context, _ = merge(parts, head_size, True)
    out_ref[...] = (middle_ref[...] + dot(context.astype(bf16), weight_ref[...])).astype(bf16)


def step(
    token_ids,
    parents,
    embedding,
    self_gain,
    query_weight,
    key_weight,
    value_weight,
    output_weight,
    past_keys,
    past_values,
    cross_gain,
    cross_query,
    cross_output,
    image_keys,
    image_values,
):
    images, _, width_here = past_keys.shape
    slab, width = embedding.shape
    head_size = width // HEADS
    groups = lax.axis_size("dp") // BEAMS
    patches = lax.axis_size("patch")
    group_rows = BEAMS * images
    half = group_rows // 2
    smem = pl.BlockSpec(memory_space=pltpu.SMEM)
    vmem = pl.BlockSpec(memory_space=pltpu.VMEM)

    weights = {0: output_weight}
    mask = patches // 2
    while mask > 1:
        weights |= {k ^ mask: swap(piece, "patch", mask) for k, piece in weights.items()}
        mask //= 2

    table = embedding.reshape(slab // SUB, SUB, width)
    table = pltpu.with_memory_space_constraint(table, pltpu.HBM)
    ids = pltpu.with_memory_space_constraint(token_ids, pltpu.HBM)

    def gather(slots):
        return pl.pallas_call(
            functools.partial(gather_kernel, slots=slots, images=images, slab=slab),
            out_shape=[jax.ShapeDtypeStruct((half, width), bf16)] * len(slots),
            in_specs=[pl.BlockSpec(memory_space=pltpu.HBM)] * 2,
            out_specs=[vmem] * len(slots),
            scratch_shapes=[
                pltpu.SMEM(token_ids.shape, jnp.int32),
                pltpu.VMEM((len(slots) * half, SUB, width), bf16),
                pltpu.SemaphoreType.DMA,
                pltpu.SemaphoreType.DMA,
            ],
            compiler_params=params(8),
        )(ids, table)

    if groups > 1:
        keep = groups // 2
        sent = [swap(b, "dp", keep * BEAMS) for b in gather(range(keep, groups))]
        slots = [a + b for a, b in zip(gather(range(keep)), sent)]
    else:
        slots = gather(range(groups))
    while len(slots) > 1:
        keep = len(slots) // 2
        slots = [a + swap(b, "dp", keep * BEAMS) for a, b in zip(slots[:keep], slots[keep:])]
    own = slots[0]
    own = own + sum(swap(own, "dp", k) for k in range(1, BEAMS))
    other = swap(own, "patch", 1)
    weights |= {k ^ 1: swap(piece, "patch", 1) for k, piece in weights.items()}
    outputs = [weights[k] for k in range(patches)]

    context, new_key, new_value = pl.pallas_call(
        functools.partial(self_kernel, head_size=head_size),
        out_shape=[
            jax.ShapeDtypeStruct((group_rows, width_here), bf16),
            jax.ShapeDtypeStruct((images, width_here), bf16),
            jax.ShapeDtypeStruct((images, width_here), bf16),
        ],
        in_specs=[smem] + [vmem] * 8,
        out_specs=[vmem] * 3,
        scratch_shapes=[pltpu.VMEM((width_here // LANES, group_rows, LANES), f32)] * 2,
        compiler_params=params(16),
        name="self_attention",
    )(parents, own, other, self_gain.reshape(1, width), query_weight, key_weight, value_weight,
      past_keys, past_values)
    context = context + sum(swap(context, "dp", k) for k in range(1, BEAMS))
    contexts = [context] + [swap(context, "patch", k) for k in range(1, patches)]

    patch_count = image_keys.shape[2]
    score_rows = images // PAIR * HEADS * SUB
    middle, *messages = pl.pallas_call(
        functools.partial(cross_kernel, pieces=patches, head_size=head_size),
        out_shape=[jax.ShapeDtypeStruct((images, width), f32)]
        + [jax.ShapeDtypeStruct((images, width + LANES), bf16)] * BEAMS,
        in_specs=[vmem] * (2 * patches + 6),
        out_specs=[vmem] * (1 + BEAMS),
        scratch_shapes=[
            pltpu.VMEM((width // LANES, group_rows, LANES), f32),
            pltpu.VMEM((width // LANES + 1, group_rows, LANES), f32),
            pltpu.VMEM((score_rows, PAIR * patch_count), f32),
            pltpu.VMEM((score_rows, PAIR * patch_count), bf16),
        ],
        compiler_params=params(24),
        name="cross_attention",
    )(*contexts, *outputs, own, other, cross_gain.reshape(1, width), cross_query, image_keys,
      image_values)
    parts = [swap(messages[k], "dp", k) for k in range(BEAMS - 1, 0, -1)] + [messages[0]]
    part = pl.pallas_call(
        functools.partial(merge_kernel, head_size=head_size),
        out_shape=jax.ShapeDtypeStruct((images, width + LANES), bf16),
        in_specs=[vmem] * BEAMS,
        out_specs=vmem,
        compiler_params=params(8),
        name="merge",
    )(*parts)
    parts = [part] + [swap(part, "patch", k) for k in range(1, patches)]
    hidden = pl.pallas_call(
        functools.partial(final_kernel, head_size=head_size),
        out_shape=jax.ShapeDtypeStruct((images, width), bf16),
        in_specs=[vmem] * (patches + 2),
        out_specs=vmem,
        compiler_params=params(8),
        name="final",
    )(*parts, middle, cross_output)
    return (hidden, new_key, new_value)


def solution(mesh):
    in_specs = (
        P(),
        P(),
        P("dp", None),
        P(),
        P(None, "patch"),
        P(None, "patch"),
        P(None, "patch"),
        P("patch", None),
        P("dp", None, "patch"),
        P("dp", None, "patch"),
        P(),
        P(),
        P(),
        P("dp", None, "patch", None),
        P("dp", None, "patch", None),
    )
    out_specs = (P("dp", None), P("dp", "patch"), P("dp", "patch"))
    return jax.shard_map(step, mesh=mesh, in_specs=in_specs, out_specs=out_specs, check_vma=False)
```

```python
import functools
import math

import jax
import jax.numpy as jnp
from jax import lax
from jax.experimental import pallas as pl
from jax.experimental.pallas import tpu as pltpu
from jax.sharding import PartitionSpec as P


HEADS = 16
BEAMS = 4
SUB = 8
PAIR = SUB // BEAMS
LANES = 128
LOW = -1e30

f32 = jnp.float32
bf16 = jnp.bfloat16


def swap(value, axis, mask):
    pairs = [(source, source ^ mask) for source in range(lax.axis_size(axis))]
    return lax.ppermute(value, axis, pairs)


def cross(value, mask):
    patches = lax.axis_size("patch")
    devices = lax.axis_size("dp") * patches
    pairs = [(source, source ^ (mask * patches + 1)) for source in range(devices)]
    return lax.ppermute(value, ("dp", "patch"), pairs)


def params(mib):
    return pltpu.CompilerParams(vmem_limit_bytes=mib * 2**20)


def dot(a, b):
    return jnp.dot(a, b, preferred_element_type=f32)


def dot_nt(a, b):
    return lax.dot_general(a, b, (((1,), (1,)), ((), ())), preferred_element_type=f32)


def normalize(inputs, gains):
    factor = lax.rsqrt(jnp.mean(inputs * inputs, axis=-1, keepdims=True) + 1e-06)
    return (inputs * factor * gains.astype(f32)).astype(bf16)


def place():
    position = lax.axis_index("dp")
    return position // BEAMS, position % BEAMS, lax.axis_index("patch") % 2


def join_halves(own_ref, other_ref, core):
    own = own_ref[...].astype(f32)
    other = other_ref[...].astype(f32)
    return jnp.concatenate([jnp.where(core == 1, own, other), jnp.where(core == 1, other, own)], 0)


def gather_kernel(ids_ref, table_ref, *refs, slots, images, slab):
    outs, (ids_smem, blocks, ids_sem, sem) = refs[:-4], refs[-4:]
    pltpu.make_async_copy(ids_ref, ids_smem, ids_sem).start()
    group, _, core = place()
    first = lax.axis_index("dp") * slab
    here = images // 2
    rows = here * BEAMS
    width = blocks.shape[2]
    locals_, mine = [], []
    pltpu.make_async_copy(ids_ref, ids_smem, ids_sem).wait()
    for slot in slots:
        base = (group ^ slot) * (BEAMS * images) + core * here
        for k in range(rows):
            local = ids_smem[base + (k % BEAMS) * images + k // BEAMS] - first
            held = jnp.clip(local, 0, slab - 1)
            source = table_ref.at[lax.shift_right_logical(held, int(math.log2(SUB)))]
            pltpu.make_async_copy(source, blocks.at[len(mine)], sem).start()
            locals_.append(held & (SUB - 1))
            mine.append(local == held)
    pltpu.make_async_copy(blocks, blocks, sem).wait()
    sub = lax.broadcasted_iota(jnp.int32, (SUB, width), 0)
    for out, begin in zip(outs, range(0, len(mine), rows)):
        for base in range(0, rows, 2 * SUB):
            tiles = []
            for tile in (base, base + SUB):
                packed = jnp.zeros((SUB, width), f32)
                for k in range(SUB):
                    at = begin + tile + k
                    turned = pltpu.roll(blocks[at].astype(f32), (k + SUB - locals_[at]) & (SUB - 1), 0)
                    packed = jnp.where(jnp.logical_and(sub == k, mine[at]), turned, packed)
                tiles.append(packed)
            out[base : base + 2 * SUB, :] = jnp.concatenate(tiles, 0).astype(bf16)


def spread(rows8, heads, head_size):
    owner = lax.broadcasted_iota(jnp.int32, rows8.shape, 1) // head_size
    return jnp.concatenate([jnp.where(owner == h, rows8, 0.0) for h in range(heads)], 0)


def fold(wide, heads, head_size):
    owner = lax.broadcasted_iota(jnp.int32, (SUB, wide.shape[1]), 1) // head_size
    folded = wide[:SUB]
    for h in range(1, heads):
        folded = jnp.where(owner == h, wide[h * SUB : (h + 1) * SUB], folded)
    return folded


def same_image(shape, length):
    row = lax.broadcasted_iota(jnp.int32, shape, 0) % SUB // BEAMS
    return row == lax.broadcasted_iota(jnp.int32, shape, 1) // length


def self_kernel(parents_ref, own_ref, other_ref, gain_ref, wq_ref, wk_ref, wv_ref, pk_ref, pv_ref,
                context_ref, key_ref, value_ref, key_scr, value_scr, *, head_size):
    group, beam, core = place()
    images, length, width = pk_ref.shape
    heads = width // head_size
    scaling = 1.0 / math.sqrt(head_size)
    normed = normalize(join_halves(own_ref, other_ref, core), gain_ref[...])
    queries = dot(normed, wq_ref[...]).astype(bf16).astype(f32)
    keys = dot(normed, wk_ref[...]).astype(bf16).astype(f32)
    values = dot(normed, wv_ref[...]).astype(bf16).astype(f32)
    for first in range(0, width, LANES):
        key_scr[first // LANES] = keys[:, first : first + LANES]
        value_scr[first // LANES] = values[:, first : first + LANES]
    for first in range(0, width, LANES):
        mine = pl.ds(beam, images, stride=BEAMS)
        key_ref[:, first : first + LANES] = key_scr[first // LANES, mine, :].astype(bf16)
        value_ref[:, first : first + LANES] = value_scr[first // LANES, mine, :].astype(bf16)
    shape = (BEAMS * images, parents_ref.shape[1])
    row = lax.broadcasted_iota(jnp.int32, shape, 0)
    row = (group * BEAMS + row % BEAMS) * images + row // BEAMS
    chosen = jnp.logical_and(row == lax.broadcasted_iota(jnp.int32, shape, 1), parents_ref[...] == beam)
    lives = jnp.sum(chosen.astype(f32), axis=-1, keepdims=True)
    pairs = images // PAIR
    seen = same_image((heads * SUB, PAIR * length), length)
    scores, owns = [], []
    for j in range(pairs):
        q = spread(queries[j * SUB : (j + 1) * SUB], heads, head_size)
        k = jnp.concatenate([keys[j * SUB : (j + 1) * SUB]] * heads, 0)
        past = pk_ref[j * PAIR : (j + 1) * PAIR].reshape(PAIR * length, width)
        scores.append(dot_nt(q.astype(bf16), past))
        owns.append(jnp.sum(q * k, axis=-1, keepdims=True) * scaling)
    weights, own_weights, totals = [], [], []
    for j in range(pairs):
        s = jnp.where(seen, scores[j] * scaling, LOW)
        peak = jnp.maximum(jnp.max(s, axis=-1, keepdims=True), owns[j])
        power = jnp.exp(s - peak)
        own_power = jnp.exp(owns[j] - peak)
        totals.append(jnp.sum(power, axis=-1, keepdims=True) + own_power)
        weights.append(power.astype(bf16))
        own_weights.append(own_power.astype(bf16).astype(f32))
    done = []
    for j in range(pairs):
        past = pv_ref[j * PAIR : (j + 1) * PAIR].reshape(PAIR * length, width)
        v = jnp.concatenate([values[j * SUB : (j + 1) * SUB]] * heads, 0)
        summed = (dot(weights[j], past) + own_weights[j] * v) / totals[j]
        folded = fold(summed, heads, head_size)
        done.append(jnp.where(lives[j * SUB : (j + 1) * SUB] > 0.5, folded, 0.0))
    context_ref[...] = jnp.concatenate(done, 0).astype(bf16)


def cross_kernel(*refs, pieces, head_size):
    contexts = refs[:pieces]
    outputs = refs[pieces : 2 * pieces]
    own_ref, other_ref, gain_ref, query_ref, ik_ref, iv_ref = refs[2 * pieces : 2 * pieces + 6]
    middle_ref, *messages = refs[2 * pieces + 6 : 2 * pieces + 7 + BEAMS]
    mid_scr, sum_scr, s_scr, p_scr = refs[2 * pieces + 7 + BEAMS :]
    _, beam, core = place()
    _, images, length, width = ik_ref.shape
    scaling = 1.0 / math.sqrt(head_size)
    middle = join_halves(own_ref, other_ref, core)
    for piece in range(pieces):
        middle = middle + dot(contexts[piece][...], outputs[piece][...])
    mine = pl.ds(beam, images, stride=BEAMS)
    for first in range(0, width, LANES):
        mid_scr[first // LANES] = middle[:, first : first + LANES]
    for first in range(0, width, LANES):
        middle_ref[:, first : first + LANES] = mid_scr[first // LANES, mine, :]
    probes = dot(normalize(middle, gain_ref[...]), query_ref[...]).astype(bf16).astype(f32)
    pairs = images // PAIR
    block = min(width, 2 * LANES)
    heads = block // head_size
    blocks = width // block
    rows = heads * SUB
    for j in range(pairs):
        for n in range(blocks):
            at = slice(n * block, (n + 1) * block)
            q = spread(probes[j * SUB : (j + 1) * SUB, at], heads, head_size).astype(bf16)
            past = ik_ref[0, j * PAIR : (j + 1) * PAIR, :, at].reshape(PAIR * length, block)
            s_scr[(j * blocks + n) * rows : (j * blocks + n + 1) * rows, :] = dot_nt(q, past)
    seen = same_image((rows, PAIR * length), length)
    lane = lax.broadcasted_iota(jnp.int32, (SUB, LANES), 1)
    for j in range(pairs):
        stats = jnp.zeros((SUB, LANES), f32)
        for n in range(blocks):
            at = slice((j * blocks + n) * rows, (j * blocks + n + 1) * rows)
            s = jnp.where(seen, s_scr[at, :] * scaling, LOW)
            peak = jnp.max(s, axis=-1, keepdims=True)
            power = jnp.exp(s - peak)
            total = jnp.sum(power, axis=-1, keepdims=True)
            p_scr[at, :] = power.astype(bf16)
            for h in range(heads):
                head = n * heads + h
                stats = jnp.where(lane == head, peak[h * SUB : (h + 1) * SUB], stats)
                stats = jnp.where(lane == HEADS + head, total[h * SUB : (h + 1) * SUB], stats)
        sum_scr[width // LANES, j * SUB : (j + 1) * SUB, :] = stats
    for j in range(pairs):
        for n in range(blocks):
            at = slice((j * blocks + n) * rows, (j * blocks + n + 1) * rows)
            past = iv_ref[0, j * PAIR : (j + 1) * PAIR, :, n * block : (n + 1) * block]
            summed = fold(dot(p_scr[at, :], past.reshape(PAIR * length, block)), heads, head_size)
            for part in range(block // LANES):
                sum_scr[n * (block // LANES) + part, j * SUB : (j + 1) * SUB, :] = summed[
                    :, part * LANES : (part + 1) * LANES
                ]
    for k in range(BEAMS):
        theirs = pl.ds(beam ^ k, images, stride=BEAMS)
        for part in range(width // LANES):
            messages[k][:, part * LANES : (part + 1) * LANES] = sum_scr[part, theirs, :].astype(bf16)
        messages[k][:, width:] = pack(sum_scr[width // LANES, theirs, :])


def split(value, terms):
    out = []
    for _ in range(terms):
        out.append(value.astype(bf16))
        value = value - out[-1].astype(f32)
    return out


def pack(stats):
    lane = lax.broadcasted_iota(jnp.int32, stats.shape, 1)
    packed = jnp.zeros(stats.shape, f32)
    for at, term in enumerate(split(stats, 3)):
        term = term.astype(f32)
        tall = pltpu.roll(term, 2 * at * HEADS, 1) if at else term
        inside = jnp.logical_and(lane >= 2 * at * HEADS, lane < 2 * (at + 1) * HEADS)
        packed = jnp.where(inside, tall, packed)
    return packed.astype(bf16)


def merge(parts, head_size, last):
    rows = parts[0].shape[0]
    width = parts[0].shape[1] - LANES
    lane = lax.broadcasted_iota(jnp.int32, (rows, LANES), 1)
    peaks, totals = [], []
    for part in parts:
        stat = part[:, width:].astype(f32)
        stat = stat + pltpu.roll(stat, LANES - 2 * HEADS, 1) + pltpu.roll(stat, LANES - 4 * HEADS, 1)
        peaks.append(stat)
        totals.append(pltpu.roll(stat, LANES - HEADS, 1))
    peak = functools.reduce(jnp.maximum, peaks)
    scales = [jnp.where(lane < HEADS, jnp.exp(p - peak), 0.0) for p in peaks]
    total = sum(scale * t for scale, t in zip(scales, totals))
    if last:
        total = jnp.where(lane < HEADS, total, 1.0)
        scales = [scale / total for scale in scales]
    row = lax.broadcasted_iota(jnp.int32, (LANES, width), 0)
    owner = lax.broadcasted_iota(jnp.int32, (LANES, width), 1) // head_size
    widen = (row == owner).astype(bf16)
    high, low = split(jnp.concatenate(scales, 0), 2)
    wide = dot(jnp.concatenate([high, low], 0), widen)
    many = len(parts) * rows
    wide = wide[:many] + wide[many:]
    sums = 0.0
    for k, part in enumerate(parts):
        sums = sums + part[:, :width].astype(f32) * wide[k * rows : (k + 1) * rows]
    stats = jnp.where(lane < HEADS, peak, pltpu.roll(total, HEADS, 1))
    return sums, jnp.where(lane < 2 * HEADS, stats, 0.0)


def merge_kernel(*refs, head_size):
    parts, out_ref = [ref[...] for ref in refs[:-1]], refs[-1]
    sums, stats = merge(parts, head_size, False)
    width = sums.shape[1]
    out_ref[:, :width] = sums.astype(bf16)
    out_ref[:, width:] = pack(stats)


def final_kernel(*refs, head_size):
    parts = [ref[...] for ref in refs[:-3]]
    middle_ref, weight_ref, out_ref = refs[-3:]
    context, _ = merge(parts, head_size, True)
    out_ref[...] = (middle_ref[...] + dot(context.astype(bf16), weight_ref[...])).astype(bf16)


def step(
    token_ids,
    parents,
    embedding,
    self_gain,
    query_weight,
    key_weight,
    value_weight,
    output_weight,
    past_keys,
    past_values,
    cross_gain,
    cross_query,
    cross_output,
    image_keys,
    image_values,
):
    images, _, width_here = past_keys.shape
    slab, width = embedding.shape
    head_size = width // HEADS
    groups = lax.axis_size("dp") // BEAMS
    patches = lax.axis_size("patch")
    group_rows = BEAMS * images
    half = group_rows // 2
    vmem = pl.BlockSpec(memory_space=pltpu.VMEM)

    weights = {0: output_weight}
    mask = patches // 2
    while mask > 1:
        weights |= {k ^ mask: swap(piece, "patch", mask) for k, piece in weights.items()}
        mask //= 2

    table = embedding.reshape(slab // SUB, SUB, width)
    table = pltpu.with_memory_space_constraint(table, pltpu.HBM)
    ids = pltpu.with_memory_space_constraint(token_ids, pltpu.HBM)

    def gather(slots):
        return pl.pallas_call(
            functools.partial(gather_kernel, slots=slots, images=images, slab=slab),
            out_shape=[jax.ShapeDtypeStruct((half, width), bf16)] * len(slots),
            in_specs=[pl.BlockSpec(memory_space=pltpu.HBM)] * 2,
            out_specs=[vmem] * len(slots),
            scratch_shapes=[
                pltpu.SMEM(token_ids.shape, jnp.int32),
                pltpu.VMEM((len(slots) * half, SUB, width), bf16),
                pltpu.SemaphoreType.DMA,
                pltpu.SemaphoreType.DMA,
            ],
            compiler_params=params(8),
        )(ids, table)

    if groups > 1:
        keep = groups // 2
        sent = [swap(b, "dp", keep * BEAMS) for b in gather(range(keep, groups))]
        slots = [a + b for a, b in zip(gather(range(keep)), sent)]
    else:
        slots = gather(range(groups))
    while len(slots) > 1:
        keep = len(slots) // 2
        slots = [a + swap(b, "dp", keep * BEAMS) for a, b in zip(slots[:keep], slots[keep:])]
    own = slots[0]
    own = sum(cross(own, k) for k in range(BEAMS))
    other = swap(own, "patch", 1)
    weights |= {k ^ 1: swap(piece, "patch", 1) for k, piece in weights.items()}
    outputs = [weights[k ^ 1] for k in range(patches)]

    context, new_key, new_value = pl.pallas_call(
        functools.partial(self_kernel, head_size=head_size),
        out_shape=[
            jax.ShapeDtypeStruct((group_rows, width_here), bf16),
            pltpu.VMEM((images, width_here), bf16),
            pltpu.VMEM((images, width_here), bf16),
        ],
        in_specs=[vmem] * 9,
        out_specs=[vmem] * 3,
        scratch_shapes=[pltpu.VMEM((width_here // LANES, group_rows, LANES), f32)] * 2,
        compiler_params=params(16),
        name="self_attention",
    )(parents.reshape(1, -1), own, other, self_gain.reshape(1, width), query_weight, key_weight, value_weight,
      past_keys, past_values)
    context = sum(cross(context, k) for k in range(BEAMS))
    contexts = [context] + [swap(context, "patch", k) for k in range(1, patches)]

    patch_count = image_keys.shape[2]
    score_rows = images // PAIR * HEADS * SUB
    middle, *messages = pl.pallas_call(
        functools.partial(cross_kernel, pieces=patches, head_size=head_size),
        out_shape=[jax.ShapeDtypeStruct((images, width), f32)]
        + [jax.ShapeDtypeStruct((images, width + LANES), bf16)] * BEAMS,
        in_specs=[vmem] * (2 * patches + 6),
        out_specs=[vmem] * (1 + BEAMS),
        scratch_shapes=[
            pltpu.VMEM((width // LANES, group_rows, LANES), f32),
            pltpu.VMEM((width // LANES + 1, group_rows, LANES), f32),
            pltpu.VMEM((score_rows, PAIR * patch_count), f32),
            pltpu.VMEM((score_rows, PAIR * patch_count), bf16),
        ],
        compiler_params=params(24),
        name="cross_attention",
    )(*contexts, *outputs, own, other, cross_gain.reshape(1, width), cross_query, image_keys,
      image_values)
    parts = [cross(messages[k], k) for k in range(BEAMS - 1, 0, -1)] + [messages[0]]
    part = pl.pallas_call(
        functools.partial(merge_kernel, head_size=head_size),
        out_shape=jax.ShapeDtypeStruct((images, width + LANES), bf16),
        in_specs=[vmem] * BEAMS,
        out_specs=vmem,
        compiler_params=params(8),
        name="merge",
    )(*parts)
    parts = [part] + [swap(part, "patch", k) for k in range(1, patches)]
    hidden = pl.pallas_call(
        functools.partial(final_kernel, head_size=head_size),
        out_shape=jax.ShapeDtypeStruct((images, width), bf16),
        in_specs=[vmem] * (patches + 2),
        out_specs=vmem,
        compiler_params=params(8),
        name="final",
    )(*parts, middle, cross_output)
    return (hidden, new_key, new_value)


def solution(mesh):
    in_specs = (
        P(),
        P(),
        P("dp", None),
        P(),
        P(None, "patch"),
        P(None, "patch"),
        P(None, "patch"),
        P("patch", None),
        P("dp", None, "patch"),
        P("dp", None, "patch"),
        P(),
        P(),
        P(),
        P("dp", None, "patch", None),
        P("dp", None, "patch", None),
    )
    out_specs = (P("dp", None), P("dp", "patch"), P("dp", "patch"))
    return jax.shard_map(step, mesh=mesh, in_specs=in_specs, out_specs=out_specs, check_vma=False)
```
